1024 devices in a mesh: mem: 64 (over x_hi, y, core), patch: 16 (over x_lo, z).
Axes of the slice: x: 8 (x_hi: 4, x_lo: 2; x = x_hi * 2 + x_lo), y: 8, z: 8, core: 2. Of those that a mesh axis runs over, the one named last changes fastest.
Arguments:
- ens: bfloat16 [2, 256, 8, 131072], P(None, 'mem', None, 'patch'), may hold values from -6 to 6
- obs_pert: bfloat16 [2, 256, 8192], P(None, None, 'patch'), may hold values from -6 to 6
- obs_innov: bfloat16 [2, 8192], P(None, 'patch'), may hold values from -6 to 6
- obs_pos: bfloat16 [2, 8192], P(None, 'patch'), may hold values from 0 to 1
- obs_prec: bfloat16 [2, 8192], P(None, 'patch'), may hold values from 0.25 to 4
Outputs:
- analysed: bfloat16 [2, 256, 8, 131072], P(None, 'mem', None, 'patch')
The draws below stay inside these ranges and needn't reach their ends.
All inputs are finite; a program needn't handle non-finite values.
Results may differ from the reference program's by a relative error of at most 0.0058.
Values may be sent and summed in bfloat16 or wider, within the bound.
No kernel may reach another device: no remote copies, remote signals or barrier semaphores. Data moves between devices by JAX's collectives and lax.ppermute only.
A program may use at most 64 MiB of HBM per device.

```python
import math
import jax
import jax.numpy as jnp
from jax import lax

K = 256
SLABS = 2
LEVELS = 8
GSUB = 128
NOB_DEV = 512
NS_ITERS = 2
GCOL = 131072
NOBS = 8192
N_MEM = 64
N_PATCH = 16


def block_scale(stream_key, shape, pieces, least, high):
    factor_of = 1.0
    for dim, parts in pieces:
        draws = jax.random.uniform(jax.random.fold_in(jax.random.fold_in(stream_key, 6), dim), (parts,), jnp.float32, least / len(pieces), high / len(pieces))
        factor_of = factor_of * jnp.repeat(jnp.exp(draws), shape[dim] // parts).reshape((-1,) + (1,) * (len(shape) - 1 - dim))
    return factor_of


def noise(stream_key, shape, width, reach, split=(), held_as=jnp.bfloat16):
    values = jax.random.normal(stream_key, shape, jnp.float32) * width
    if len(split) > 0:
        values = block_scale(stream_key, shape, split, -0.22, 0.18) * values
    return jnp.clip(values, min=-reach, max=reach).astype(held_as)


def setup_inputs(seed: int = 0) -> dict:
    splits = jax.random.split(jax.random.key(seed), 6)
    return {
        "ens": noise(splits[0], (SLABS, K, LEVELS, GCOL), 1.0, 6.0, ((1, 64), (3, 16))),
        "obs_pert": noise(splits[1], (SLABS, K, NOBS), 1.0, 6.0, ((2, 16),)),
        "obs_innov": noise(splits[2], (SLABS, NOBS), 1.0, 6.0, ((1, 16),)),
        "obs_pos": jnp.clip(1.0 * jax.random.uniform(splits[3], (SLABS, NOBS), jnp.float32) ** block_scale(splits[3], (SLABS, NOBS), ((1, 16),), -0.2, 0.2), 0.0, 1.0).astype(jnp.bfloat16),
        "obs_prec": jnp.clip(jnp.exp(math.log(4.0) - 2.7725887 * jax.random.uniform(splits[4], (SLABS, NOBS), jnp.float32) ** block_scale(splits[4], (SLABS, NOBS), ((1, 16),), -0.2, 0.2)), 0.25, 4.0).astype(jnp.bfloat16),
    }


loc_scale = 0.5

def matmul(left, right):
    return jnp.dot(left, right, precision=lax.Precision.HIGHEST)

def region_weights(deviations, innovation, position, precision, center):
    members = deviations.shape[0]
    taper = jnp.exp(-0.5 * ((position - center) / loc_scale) ** 2)
    obs_weight = taper * precision.astype(jnp.float32)
    scaled = (deviations.astype(jnp.float32) * obs_weight[None, :]).astype(jnp.bfloat16)
    gram_sum = jnp.dot(scaled, deviations.T, preferred_element_type=jnp.float32)
    innov_sum = jnp.dot(scaled, innovation, preferred_element_type=jnp.float32)
    identity = jnp.eye(members, dtype=jnp.float32)
    system = (members - 1.0) * identity + gram_sum
    frobenius = jnp.sqrt(jnp.sum(system * system))
    current = system / frobenius
    inverse = identity
    for sweep in range(NS_ITERS):
        factor = 1.5 * identity - 0.5 * matmul(inverse, current)
        if sweep + 1 < NS_ITERS:
            current = matmul(current, factor)
        inverse = matmul(factor, inverse)
    inner = jnp.dot(inverse, innov_sum, precision=lax.Precision.HIGHEST)
    mean_weight = jnp.dot(inverse, inner, precision=lax.Precision.HIGHEST) / frobenius
    spread = inverse * jnp.sqrt((members - 1.0) / frobenius)
    return (spread + mean_weight[:, None]).astype(jnp.bfloat16)

def three_patches(values, axis):
    return jnp.concatenate([jnp.roll(values, 1, axis=axis), values, jnp.roll(values, -1, axis=axis)], axis=-1)

def reference(ens, obs_pert, obs_innov, obs_pos, obs_prec):
    members = obs_pert.shape[1]
    slab_count = ens.shape[0]
    level_count = ens.shape[2]
    deviations = three_patches(obs_pert.reshape(slab_count, members, N_PATCH, NOB_DEV), 2)
    deviations = deviations.transpose(0, 2, 1, 3).reshape(slab_count * N_PATCH, members, 3 * NOB_DEV)
    innovation = three_patches(obs_innov.reshape(slab_count, N_PATCH, NOB_DEV), 1).reshape(slab_count * N_PATCH, 3 * NOB_DEV)
    offsets = jnp.repeat(jnp.array([-1.0, 0.0, 1.0], jnp.float32), NOB_DEV)
    position = three_patches(obs_pos.astype(jnp.float32).reshape(slab_count, N_PATCH, NOB_DEV), 1) + offsets
    position = position.reshape(slab_count * N_PATCH, 3 * NOB_DEV)
    precision = three_patches(obs_prec.reshape(slab_count, N_PATCH, NOB_DEV), 1).reshape(slab_count * N_PATCH, 3 * NOB_DEV)
    centers = (jnp.arange(N_MEM, dtype=jnp.float32) + 0.5) / N_MEM

    def one_patch(items):
        dev_rows, innov_row, pos_row, prec_row = items
        return jax.vmap(lambda center: region_weights(dev_rows, innov_row, pos_row, prec_row, center))(centers)
    weights = lax.map(one_patch, (deviations, innovation, position, precision))
    weights = weights.reshape(slab_count, N_PATCH, N_MEM, members, members).transpose(1, 0, 2, 3, 4)
    blocks = ens.reshape(slab_count, members, level_count, N_PATCH, N_MEM, GSUB).transpose(3, 0, 1, 2, 4, 5)

    def apply_patch(items):
        block, wts = items
        average = lax.optimization_barrier(jnp.mean(block.astype(jnp.float32), axis=1, keepdims=True))
        anomaly = (block.astype(jnp.float32) - average).astype(jnp.bfloat16)
        mixed = jnp.einsum('sjlmg,smjk->sklmg', anomaly.astype(jnp.float32), wts.astype(jnp.float32))
        return (average + mixed).astype(jnp.bfloat16)
    result = lax.map(apply_patch, (blocks, weights))
    return result.transpose(1, 2, 3, 0, 4, 5).reshape(slab_count, members, level_count, N_PATCH * N_MEM * GSUB)
```

```python
import jax
import jax.numpy as jnp
from jax import lax
from jax.sharding import PartitionSpec as P


NS_ITERS = 2
MEM = "mem"
LOC_SCALE = 0.5


def halo(block):
    count = lax.axis_size("patch")
    forward = [(i, (i + 1) % count) for i in range(count)]
    backward = [(target, source) for source, target in forward]
    low = lax.ppermute(block, "patch", forward)
    high = lax.ppermute(block, "patch", backward)
    return low, high


def matmul(left, right):
    return jnp.einsum("sij,sjk->sik", left, right, precision=lax.Precision.HIGHEST)


def local_terms(deviations, innovation, position, precision, offset, center):
    distance = position.astype(jnp.float32) + offset - center
    taper = jnp.exp(-0.5 * (distance / LOC_SCALE) ** 2)
    obs_weight = taper * precision.astype(jnp.float32)
    scaled = (deviations.astype(jnp.float32) * obs_weight[:, None, :]).astype(jnp.bfloat16)
    gram_sum = jnp.einsum("skn,sjn->skj", scaled, deviations, preferred_element_type=jnp.float32)
    innov_sum = jnp.einsum("skn,sn->sk", scaled, innovation, preferred_element_type=jnp.float32)
    return gram_sum, innov_sum


def transform_weights(gram_sum, innov_sum, members):
    identity = jnp.eye(members, dtype=jnp.float32)[None]
    system = (members - 1.0) * identity + gram_sum
    frobenius = jnp.sqrt(jnp.sum(system * system, axis=(1, 2)))[:, None, None]
    current = system / frobenius
    inverse = jnp.broadcast_to(identity, system.shape)
    for sweep in range(NS_ITERS):
        factor = 1.5 * identity - 0.5 * matmul(inverse, current)
        if sweep + 1 < NS_ITERS:
            current = matmul(current, factor)
        inverse = matmul(factor, inverse)
    inner = jnp.einsum("sjk,sk->sj", inverse, innov_sum, precision=lax.Precision.HIGHEST)
    mean_weight = (
        jnp.einsum("sjk,sk->sj", inverse, inner, precision=lax.Precision.HIGHEST)
        / frobenius[:, :, 0]
    )
    spread = inverse * jnp.sqrt((members - 1.0) / frobenius)
    return (spread + mean_weight[:, :, None]).astype(jnp.bfloat16)


def analyse(block, weights):
    average = jnp.mean(block.astype(jnp.float32), axis=1, keepdims=True)
    anomaly = (block.astype(jnp.float32) - average).astype(jnp.bfloat16)
    mixed = jnp.einsum("sjlg,sjk->sklg", anomaly, weights, preferred_element_type=jnp.float32)
    return (average + mixed).astype(jnp.bfloat16)


def on_device(ens, obs_pert, obs_innov, obs_pos, obs_prec):
    slabs, own, levels, _ = ens.shape
    members = obs_pert.shape[1]
    ranks = lax.axis_size(MEM)
    pieces = jnp.moveaxis(ens.reshape(slabs, own, levels, ranks, -1), 3, 0)
    gathered = lax.all_to_all(pieces, MEM, 0, 0, tiled=True)
    center = (lax.axis_index(MEM).astype(jnp.float32) + 0.5) / ranks
    stacked = jnp.concatenate(
        [obs_pert, obs_innov[:, None, :], obs_pos[:, None, :], obs_prec[:, None, :]], axis=1
    )
    low, high = halo(stacked)
    padded = jnp.concatenate([low, stacked, high], axis=2)
    offsets = jnp.repeat(jnp.array([-1.0, 0.0, 1.0], jnp.float32), obs_pert.shape[2])
    gram_sum, innov_sum = local_terms(
        padded[:, :members],
        padded[:, members],
        padded[:, members + 1],
        padded[:, members + 2],
        offsets,
        center,
    )
    weights = transform_weights(gram_sum, innov_sum, members)
    block = jnp.moveaxis(gathered, 0, 1).reshape(slabs, members, levels, -1)
    analysed = analyse(block, weights)
    return lax.all_to_all(analysed, MEM, split_axis=1, concat_axis=3, tiled=True)


def solution(mesh):
    return jax.shard_map(
        on_device,
        mesh=mesh,
        in_specs=(
            P(None, MEM, None, "patch"),
            P(None, None, "patch"),
            P(None, "patch"),
            P(None, "patch"),
            P(None, "patch"),
        ),
        out_specs=P(None, MEM, None, "patch"),
        check_vma=False,
    )
```

```python
import jax
import jax.numpy as jnp
from jax import lax
from jax.experimental.layout import Layout, with_layout_constraint
from jax.sharding import PartitionSpec as P


NS_ITERS = 2
MEM = "mem"
LOC_SCALE = 0.5


def from_neighbours(to_next, to_previous):
    count = lax.axis_size("patch")
    forward = [(i, (i + 1) % count) for i in range(count)]
    backward = [(target, source) for source, target in forward]
    low = lax.ppermute(to_next, "patch", forward)
    high = lax.ppermute(to_previous, "patch", backward)
    return low, high


def matmul(left, right):
    return jnp.einsum("sij,sjk->sik", left, right, precision=lax.Precision.HIGHEST)


def local_terms(deviations, innovation, position, precision, offset, center):
    distance = position.astype(jnp.float32) + offset - center
    taper = jnp.exp(-0.5 * (distance / LOC_SCALE) ** 2)
    obs_weight = taper * precision.astype(jnp.float32)
    scaled = (deviations.astype(jnp.float32) * obs_weight[:, None, :]).astype(jnp.bfloat16)
    gram_sum = jnp.einsum("skn,sjn->skj", scaled, deviations, preferred_element_type=jnp.float32)
    innov_sum = jnp.einsum("skn,sn->sk", scaled, innovation, preferred_element_type=jnp.float32)
    return gram_sum, innov_sum


def packed(gram_sum, innov_sum):
    high = lax.reduce_precision(innov_sum, 8, 7)
    rows = jnp.stack([high, innov_sum - high], axis=1).astype(jnp.bfloat16)
    rows = jnp.pad(rows, ((0, 0), (0, 6), (0, 0)))
    return jnp.concatenate([gram_sum.astype(jnp.bfloat16), rows], axis=1)


def unpacked(message, members):
    gram_sum = message[:, :members].astype(jnp.float32)
    return gram_sum, jnp.sum(message[:, members : members + 2].astype(jnp.float32), axis=1)


def transform_weights(gram_sum, innov_sum, members):
    identity = jnp.eye(members, dtype=jnp.float32)[None]
    system = (members - 1.0) * identity + gram_sum
    frobenius = jnp.sqrt(jnp.sum(system * system, axis=(1, 2)))[:, None, None]
    current = system / frobenius
    inverse = 1.5 * identity - 0.5 * current
    for sweep in range(1, NS_ITERS):
        current = matmul(current, inverse if sweep == 1 else factor)
        factor = 1.5 * identity - 0.5 * matmul(inverse, current)
        inverse = matmul(factor, inverse)
    inner = jnp.einsum("sjk,sk->sj", inverse, innov_sum, precision=lax.Precision.HIGHEST)
    mean_weight = (
        jnp.einsum("sjk,sk->sj", inverse, inner, precision=lax.Precision.HIGHEST)
        / frobenius[:, :, 0]
    )
    spread = inverse * jnp.sqrt((members - 1.0) / frobenius)
    return (spread + mean_weight[:, :, None]).astype(jnp.bfloat16)


def analyse(block, weights):
    average = jnp.mean(block.astype(jnp.float32), axis=1, keepdims=True)
    anomaly = (block.astype(jnp.float32) - average).astype(jnp.bfloat16)
    mixed = jnp.einsum("sjlg,sjk->sklg", anomaly, weights, preferred_element_type=jnp.float32)
    return (average + mixed).astype(jnp.bfloat16)


def on_device(ens, obs_pert, obs_innov, obs_pos, obs_prec):
    slabs, own, levels, _ = ens.shape
    members = obs_pert.shape[1]
    ranks = lax.axis_size(MEM)
    pieces = jnp.moveaxis(ens.reshape(slabs, own, levels, ranks, -1), 3, 0)
    pieces = with_layout_constraint(pieces, Layout((0, 1, 2, 3, 4)))
    gathered = lax.all_to_all(pieces, MEM, 0, 0, tiled=True)
    center = (lax.axis_index(MEM).astype(jnp.float32) + 0.5) / ranks
    here, to_next, to_previous = (
        local_terms(obs_pert, obs_innov, obs_pos, obs_prec, offset, center)
        for offset in (0.0, -1.0, 1.0)
    )
    parts = [unpacked(m, members) for m in from_neighbours(packed(*to_next), packed(*to_previous))]
    gram_sum, innov_sum = (sum(terms) for terms in zip(here, *parts))
    weights = transform_weights(gram_sum, innov_sum, members)
    block = jnp.moveaxis(gathered, 0, 1).reshape(slabs, members, levels, -1)
    analysed = analyse(block, weights)
    return lax.all_to_all(analysed, MEM, split_axis=1, concat_axis=3, tiled=True)


def solution(mesh):
    return jax.shard_map(
        on_device,
        mesh=mesh,
        in_specs=(
            P(None, MEM, None, "patch"),
            P(None, None, "patch"),
            P(None, "patch"),
            P(None, "patch"),
            P(None, "patch"),
        ),
        out_specs=P(None, MEM, None, "patch"),
        check_vma=False,
    )
```

```python
import jax
import jax.numpy as jnp
from jax import lax
from jax.experimental.layout import Layout, with_layout_constraint
from jax.sharding import PartitionSpec as P


NS_ITERS = 2
MEM = "mem"
LOC_SCALE = 0.5
RUN = 8
EARLY_ROWS = (0,)


def sent(to_next, to_previous, chosen):
    count = lax.axis_size("patch")
    sources = [i for i in range(count) if (i % RUN in EARLY_ROWS) == chosen]
    low = lax.ppermute(to_next, "patch", [(i, (i + 1) % count) for i in sources])
    high = lax.ppermute(to_previous, "patch", [(i, (i - 1) % count) for i in sources])
    return low, high


def matmul(left, right):
    return jnp.einsum("sij,sjk->sik", left, right, precision=lax.Precision.HIGHEST)


def local_terms(deviations, innovation, position, precision, offset, center):
    distance = position.astype(jnp.float32) + offset - center
    taper = jnp.exp(-0.5 * (distance / LOC_SCALE) ** 2)
    obs_weight = taper * precision.astype(jnp.float32)
    scaled = (deviations.astype(jnp.float32) * obs_weight[:, None, :]).astype(jnp.bfloat16)
    gram_sum = jnp.einsum("skn,sjn->skj", scaled, deviations, preferred_element_type=jnp.float32)
    innov_sum = jnp.einsum("skn,sn->sk", scaled, innovation, preferred_element_type=jnp.float32)
    return gram_sum, innov_sum


def packed(gram_sum, innov_sum):
    high = lax.reduce_precision(innov_sum, 8, 7)
    rows = jnp.stack([high, innov_sum - high], axis=1).astype(jnp.bfloat16)
    rows = jnp.pad(rows, ((0, 0), (0, 6), (0, 0)))
    return jnp.concatenate([gram_sum.astype(jnp.bfloat16), rows], axis=1)


def unpacked(message, members):
    gram_sum = message[:, :members].astype(jnp.float32)
    return gram_sum, jnp.sum(message[:, members : members + 2].astype(jnp.float32), axis=1)


def transform_weights(gram_sum, innov_sum, members):
    identity = jnp.eye(members, dtype=jnp.float32)[None]
    system = (members - 1.0) * identity + gram_sum
    frobenius = jnp.sqrt(jnp.sum(system * system, axis=(1, 2)))[:, None, None]
    current = system / frobenius
    inverse = 1.5 * identity - 0.5 * current
    for sweep in range(1, NS_ITERS):
        current = matmul(current, inverse if sweep == 1 else factor)
        factor = 1.5 * identity - 0.5 * matmul(inverse, current)
        inverse = matmul(factor, inverse)
    inner = jnp.einsum("sjk,sk->sj", inverse, innov_sum, precision=lax.Precision.HIGHEST)
    mean_weight = (
        jnp.einsum("sjk,sk->sj", inverse, inner, precision=lax.Precision.HIGHEST)
        / frobenius[:, :, 0]
    )
    spread = inverse * jnp.sqrt((members - 1.0) / frobenius)
    return (spread + mean_weight[:, :, None]).astype(jnp.bfloat16)


def analyse(block, weights):
    average = jnp.mean(block.astype(jnp.float32), axis=1, keepdims=True)
    anomaly = (block.astype(jnp.float32) - average).astype(jnp.bfloat16)
    mixed = jnp.einsum("sjlg,sjk->sklg", anomaly, weights, preferred_element_type=jnp.float32)
    return (average + mixed).astype(jnp.bfloat16)


def on_device(ens, obs_pert, obs_innov, obs_pos, obs_prec):
    slabs, own, levels, _ = ens.shape
    members = obs_pert.shape[1]
    ranks = lax.axis_size(MEM)
    center = (lax.axis_index(MEM).astype(jnp.float32) + 0.5) / ranks
    here, to_next, to_previous = (
        local_terms(obs_pert, obs_innov, obs_pos, obs_prec, offset, center)
        for offset in (0.0, -1.0, 1.0)
    )
    messages = packed(*to_next), packed(*to_previous)
    received = sent(*messages, False)
    pieces = jnp.moveaxis(ens.reshape(slabs, own, levels, ranks, -1), 3, 0)
    pieces = with_layout_constraint(pieces, Layout((0, 1, 2, 3, 4)))
    gathered = lax.all_to_all(pieces, MEM, 0, 0, tiled=True)
    received += sent(*messages, True)
    parts = [unpacked(message, members) for message in received]
    gram_sum, innov_sum = (sum(terms) for terms in zip(here, *parts))
    weights = transform_weights(gram_sum, innov_sum, members)
    block = jnp.moveaxis(gathered, 0, 1).reshape(slabs, members, levels, -1)
    analysed = analyse(block, weights)
    return lax.all_to_all(analysed, MEM, split_axis=1, concat_axis=3, tiled=True)


def solution(mesh):
    return jax.shard_map(
        on_device,
        mesh=mesh,
        in_specs=(
            P(None, MEM, None, "patch"),
            P(None, None, "patch"),
            P(None, "patch"),
            P(None, "patch"),
            P(None, "patch"),
        ),
        out_specs=P(None, MEM, None, "patch"),
        check_vma=False,
    )
```

```python
import functools

import jax
import jax.numpy as jnp
from jax import lax
from jax.experimental import pallas as pl
from jax.experimental.pallas import tpu as pltpu
from jax.experimental.layout import Layout, with_layout_constraint
from jax.sharding import PartitionSpec as P


NS_ITERS = 2
MEM = "mem"
LOC_SCALE = 0.5
RUN = 8
EARLY_ROWS = (0,)


def sent(to_next, to_previous, chosen):
    count = lax.axis_size("patch")
    sources = [i for i in range(count) if (i % RUN in EARLY_ROWS) == chosen]
    low = lax.ppermute(to_next, "patch", [(i, (i + 1) % count) for i in sources])
    high = lax.ppermute(to_previous, "patch", [(i, (i - 1) % count) for i in sources])
    return low, high


def region_sums(extended, deviations, position, precision, offset, center, dtype):
    distance = position.astype(jnp.float32) + offset - center
    taper = jnp.exp(-0.5 * (distance / LOC_SCALE) ** 2)
    obs_weight = taper * precision.astype(jnp.float32)
    scaled = (deviations.astype(jnp.float32) * obs_weight[:, None, :]).astype(jnp.bfloat16)
    sums = jnp.einsum("sjn,skn->sjk", extended, scaled, preferred_element_type=jnp.float32)
    return sums.astype(dtype)


def matmul(left, right):
    return jnp.dot(left, right, precision=lax.Precision.HIGHEST, preferred_element_type=jnp.float32)


def matmul_t(left, right):
    return lax.dot_general(
        left,
        right,
        (((1,), (1,)), ((), ())),
        precision=lax.Precision.HIGHEST,
        preferred_element_type=jnp.float32,
    )


def slab_weights(sums, members):
    rows = lax.broadcasted_iota(jnp.int32, (members, members), 0)
    columns = lax.broadcasted_iota(jnp.int32, (members, members), 1)
    identity = jnp.where(rows == columns, 1.0, 0.0).astype(jnp.float32)
    system = (members - 1.0) * identity + sums[:members]
    frobenius = jnp.sqrt(jnp.sum(jnp.sum(system * system, axis=1, keepdims=True), axis=0, keepdims=True))
    current = system / frobenius
    inverse = 1.5 * identity - 0.5 * current
    factor = inverse
    for _ in range(1, NS_ITERS):
        current = matmul(current, factor)
        factor = 1.5 * identity - 0.5 * matmul(inverse, current)
        inverse = matmul(factor, inverse)
    inner = matmul_t(sums[members:], inverse)
    mean_weight = matmul_t(inverse, inner)[:, :1] / frobenius
    return (inverse * jnp.sqrt((members - 1.0) / frobenius) + mean_weight).astype(jnp.bfloat16)


def transform_weights(own, messages, earlier, late_rows):
    slabs, _, members = own.shape

    def kernel(*refs):
        own_ref, message_refs, out_ref = refs[0], refs[1 : 1 + len(messages)], refs[-1]

        def compute():
            for s in range(slabs):
                sums = own_ref[s]
                for ref in message_refs:
                    sums = sums + ref[s].astype(jnp.float32)
                out_ref[s] = slab_weights(sums, members)

        if earlier is None:
            compute()
        else:
            late = lax.axis_index("patch") % RUN
            arrives = functools.reduce(lambda a, b: a & b, [late != row for row in late_rows])
            pl.when(arrives)(compute)

            @pl.when(jnp.logical_not(arrives))
            def _():
                out_ref[...] = refs[-2][...]

    operands = (own, *messages) + (() if earlier is None else (earlier,))
    return pl.pallas_call(
        kernel,
        out_shape=jax.ShapeDtypeStruct((slabs, members, members), jnp.bfloat16),
        compiler_params=pltpu.CompilerParams(vmem_limit_bytes=16 * 2**20),
        name="weights" if earlier is None else "weights_again",
    )(*operands)


def analyse(block, weights):
    average = jnp.mean(block.astype(jnp.float32), axis=1, keepdims=True)
    anomaly = (block.astype(jnp.float32) - average).astype(jnp.bfloat16)
    mixed = jnp.einsum("sjlg,sjk->sklg", anomaly, weights, preferred_element_type=jnp.float32)
    return (average + mixed).astype(jnp.bfloat16)


def on_device(ens, obs_pert, obs_innov, obs_pos, obs_prec):
    slabs, own, levels, _ = ens.shape
    members = obs_pert.shape[1]
    ranks = lax.axis_size(MEM)
    center = (lax.axis_index(MEM).astype(jnp.float32) + 0.5) / ranks
    rows = jnp.pad(obs_innov[:, None, :], ((0, 0), (0, 7), (0, 0)))
    extended = jnp.concatenate([obs_pert, rows], axis=1)

    def sums(offset, dtype):
        return region_sums(extended, obs_pert, obs_pos, obs_prec, offset, center, dtype)

    messages = sums(-1.0, jnp.bfloat16), sums(1.0, jnp.bfloat16)
    received = sent(*messages, False)
    pieces = jnp.moveaxis(ens.reshape(slabs, own, levels, ranks, -1), 3, 0)
    pieces = with_layout_constraint(pieces, Layout((0, 1, 2, 3, 4)))
    gathered = lax.all_to_all(pieces, MEM, 0, 0, tiled=True)
    late = sent(*messages, True)
    own_sums = sums(0.0, jnp.float32)
    weights = transform_weights(own_sums, received, None, EARLY_ROWS)
    weights = transform_weights(own_sums, received + late, weights, EARLY_ROWS)
    block = jnp.moveaxis(gathered, 0, 1).reshape(slabs, members, levels, -1)
    analysed = analyse(block, weights)
    return lax.all_to_all(analysed, MEM, split_axis=1, concat_axis=3, tiled=True)


def solution(mesh):
    return jax.shard_map(
        on_device,
        mesh=mesh,
        in_specs=(
            P(None, MEM, None, "patch"),
            P(None, None, "patch"),
            P(None, "patch"),
            P(None, "patch"),
            P(None, "patch"),
        ),
        out_specs=P(None, MEM, None, "patch"),
        check_vma=False,
    )
```

```python
import functools

import jax
import jax.numpy as jnp
from jax import lax
from jax.experimental import pallas as pl
from jax.experimental.pallas import tpu as pltpu
from jax.experimental.layout import Layout, with_layout_constraint
from jax.sharding import PartitionSpec as P


NS_ITERS = 2
MEM = "mem"
LOC_SCALE = 0.5
RUN = 8
EARLY_ROWS = (0,)


def sent(message, step, late):
    count = lax.axis_size("patch")
    sources = [i for i in range(count) if (i % RUN in EARLY_ROWS) == late]
    return lax.ppermute(message, "patch", [(i, (i + step) % count) for i in sources])


def region_sums(extended, deviations, position, precision, offset, center, dtype):
    distance = position.astype(jnp.float32) + offset - center
    taper = jnp.exp(-0.5 * (distance / LOC_SCALE) ** 2)
    obs_weight = taper * precision.astype(jnp.float32)
    scaled = (deviations.astype(jnp.float32) * obs_weight[:, None, :]).astype(jnp.bfloat16)
    sums = jnp.einsum("sjn,skn->sjk", extended, scaled, preferred_element_type=jnp.float32)
    return sums.astype(dtype)


def matmul(left, right):
    return jnp.dot(left, right, precision=lax.Precision.HIGHEST, preferred_element_type=jnp.float32)


def matmul_t(left, right):
    return lax.dot_general(
        left,
        right,
        (((1,), (1,)), ((), ())),
        precision=lax.Precision.HIGHEST,
        preferred_element_type=jnp.float32,
    )


def slab_weights(sums, members):
    rows = lax.broadcasted_iota(jnp.int32, (members, members), 0)
    columns = lax.broadcasted_iota(jnp.int32, (members, members), 1)
    identity = jnp.where(rows == columns, 1.0, 0.0).astype(jnp.float32)
    system = (members - 1.0) * identity + sums[:members]
    frobenius = jnp.sqrt(jnp.sum(jnp.sum(system * system, axis=1, keepdims=True), axis=0, keepdims=True))
    current = system / frobenius
    inverse = 1.5 * identity - 0.5 * current
    factor = inverse
    for _ in range(1, NS_ITERS):
        current = matmul(current, factor)
        factor = 1.5 * identity - 0.5 * matmul(inverse, current)
        inverse = matmul(factor, inverse)
    inner = matmul_t(sums[members:], inverse)
    mean_weight = matmul_t(inverse, inner)[:, :1] / frobenius
    return (inverse * jnp.sqrt((members - 1.0) / frobenius) + mean_weight).astype(jnp.bfloat16)


def transform_weights(own, messages, earlier, late_rows):
    slabs, _, members = own.shape

    def kernel(*refs):
        own_ref, message_refs, out_ref = refs[0], refs[1 : 1 + len(messages)], refs[-1]

        def compute():
            for s in range(slabs):
                sums = own_ref[s]
                for ref in message_refs:
                    sums = sums + ref[s].astype(jnp.float32)
                out_ref[s] = slab_weights(sums, members)

        if earlier is None:
            compute()
        else:
            late = lax.axis_index("patch") % RUN
            arrives = functools.reduce(lambda a, b: a & b, [late != row for row in late_rows])
            pl.when(arrives)(compute)

            @pl.when(jnp.logical_not(arrives))
            def _():
                out_ref[...] = refs[-2][...]

    operands = (own, *messages) + (() if earlier is None else (earlier,))
    return pl.pallas_call(
        kernel,
        out_shape=jax.ShapeDtypeStruct((slabs, members, members), jnp.bfloat16),
        compiler_params=pltpu.CompilerParams(vmem_limit_bytes=16 * 2**20),
        name="weights" if earlier is None else "weights_again",
    )(*operands)


def analyse(block, weights):
    average = jnp.mean(block.astype(jnp.float32), axis=1, keepdims=True)
    anomaly = (block.astype(jnp.float32) - average).astype(jnp.bfloat16)
    mixed = jnp.einsum("sjlg,sjk->sklg", anomaly, weights, preferred_element_type=jnp.float32)
    return (average + mixed).astype(jnp.bfloat16)


def on_device(ens, obs_pert, obs_innov, obs_pos, obs_prec):
    slabs, own, levels, _ = ens.shape
    members = obs_pert.shape[1]
    ranks = lax.axis_size(MEM)
    center = (lax.axis_index(MEM).astype(jnp.float32) + 0.5) / ranks
    rows = jnp.broadcast_to(obs_innov[:, None, :], (slabs, 8, obs_innov.shape[1]))
    extended = jnp.concatenate([obs_pert, rows], axis=1)

    def sums(offset, dtype):
        return region_sums(extended, obs_pert, obs_pos, obs_prec, offset, center, dtype)

    to_next = sums(-1.0, jnp.bfloat16)
    low_first = sent(to_next, 1, False)
    pieces = jnp.moveaxis(ens.reshape(slabs, own, levels, ranks, -1), 3, 0)
    pieces = with_layout_constraint(pieces, Layout((0, 1, 2, 3, 4)))
    gathered = lax.all_to_all(pieces, MEM, 0, 0, tiled=True)
    to_previous = sums(1.0, jnp.bfloat16)
    high_first = sent(to_previous, -1, False)
    low_late = sent(to_next, 1, True)
    high_late = sent(to_previous, -1, True)
    own_sums = sums(0.0, jnp.float32)
    received = low_first, high_first
    weights = transform_weights(own_sums, received, None, EARLY_ROWS)
    received += low_late, high_late
    weights = transform_weights(own_sums, received, weights, EARLY_ROWS)
    block = jnp.moveaxis(gathered, 0, 1).reshape(slabs, members, levels, -1)
    analysed = analyse(block, weights)
    return lax.all_to_all(analysed, MEM, split_axis=1, concat_axis=3, tiled=True)


def solution(mesh):
    return jax.shard_map(
        on_device,
        mesh=mesh,
        in_specs=(
            P(None, MEM, None, "patch"),
            P(None, None, "patch"),
            P(None, "patch"),
            P(None, "patch"),
            P(None, "patch"),
        ),
        out_specs=P(None, MEM, None, "patch"),
        check_vma=False,
    )
```
